32 devices in a mesh: dp: 16 (over z, y, x), head: 2 (over core).
Axes of the slice: x: 2, y: 2, z: 4, core: 2. Of those that a mesh axis runs over, the one named last changes fastest.
Arguments:
- hidden: bfloat16 [64, 512, 3584], P(('dp', 'head')), may hold values from -6 to 6
- head_proj: bfloat16 [4, 3584, 128], P('head'), may hold values from -0.09375 to 0.09375
- head_out: bfloat16 [4, 128], P('head'), may hold values from -0.8984375 to 0.8984375
- head_ratio: int32 [4], replicated, may hold values from 2 to 7
- group_of: int32 [64], replicated, may hold values from 0 to 3, as said below
- lengths: int32 [64], P(('dp', 'head')), may hold values from 1 to 512
- token_mask: int32 [64, 512], P(('dp', 'head')), may hold values 0 or 1
Outputs:
- advantages: float32 [64, 512], P(('dp', 'head'))
The draws below stay inside these ranges and needn't reach their ends.
Inputs may be any that keep to these rules, and one draw needn't show every extreme that they name: `group_of`: every one of the 4 groups holds exactly 16 rollouts.
All inputs are finite; a program needn't handle non-finite values. No bound on the sum of `token_mask` on one device may be relied on, other than what follows from the above.
Results may differ from the reference program's by a relative error of at most 0.0026.
Values may be sent and summed in bfloat16 or wider, within the bound.
A program may use at most 64 MiB of HBM per device.

```python
import jax
import jax.numpy as jnp
from jax import lax

D = 3584
HEADS = 4
RANK = 128
GROUP = 16
LEN = 512
ROLL = 64
GROUPS = 4


def draw_group_of(key, part):
    order = jax.random.permutation(key, ROLL)
    return (order // GROUP).astype(jnp.int32)


def place_ends(result, own_key, smallest, high):
    extent = result.shape
    spot = [jax.random.randint(jax.random.fold_in(own_key, axis), (), 0, extent[axis]) for axis in range(len(extent))]
    result = result.at[tuple(spot)].set(smallest)
    longest = extent.index(max(extent))
    spot[longest] = (spot[longest] + 1) % extent[longest]
    return result.at[tuple(spot)].set(high)


def block_scale(rng, extent, split, least, top_value):
    def one(dim, blocks):
        draws = jax.random.uniform(jax.random.fold_in(jax.random.fold_in(rng, 6), dim), (blocks,), jnp.float32, least / len(split), top_value / len(split))
        return jnp.repeat(jnp.exp(draws), extent[dim] // blocks).reshape((-1,) + (1,) * (len(extent) - dim - 1))

    loudness = one(*split[0])
    for cut in split[1:]:
        loudness = loudness * one(*cut)
    return loudness


def gaussian(stream_key, extent, width, reach, pieces=(), held_as=jnp.bfloat16):
    result = jax.random.normal(stream_key, extent, jnp.float32) * width
    if len(pieces) > 0:
        result = block_scale(stream_key, extent, pieces, -0.22, 0.18) * result
    return jnp.clip(result, min=-reach, max=reach).astype(held_as)


def setup_inputs(seed: int = 0) -> dict:
    key_list = jax.random.split(jax.random.key(seed), 8)
    hidden = gaussian(key_list[0], (ROLL, LEN, D), 1.0, 6.0, ((0, 32),))
    head_proj = gaussian(key_list[1], (HEADS, D, RANK), D ** -0.5, 0.09375, ((0, 2),))
    head_out = gaussian(key_list[2], (HEADS, RANK), 0.15, 0.8984375, ((0, 2),))
    head_ratio = place_ends(jax.random.randint(key_list[3], (HEADS,), 2, 8), jax.random.fold_in(key_list[3], 1), 2, 7).astype(jnp.int32)
    group_of = draw_group_of(jax.random.fold_in(key_list[7], 71), 0)
    lengths = place_ends(jax.random.randint(key_list[5], (ROLL,), 1, LEN + 1), jax.random.fold_in(key_list[5], 1), 1, LEN).astype(jnp.int32)
    token_mask = place_ends((jax.random.randint(key_list[6], (ROLL, LEN), 0, 4) < 3).astype(jnp.int32), jax.random.fold_in(key_list[6], 1), 0, 1)
    return dict(hidden=hidden, head_proj=head_proj, head_out=head_out, head_ratio=head_ratio, group_of=group_of, lengths=lengths, token_mask=token_mask)


token_weight = 0.5
gap_weight = 0.5
clip_limit = 2.0
var_offset = 0.04

def head_mixture(head_ratio):
    ratios = head_ratio.astype(jnp.float32)
    return ratios / jnp.sum(ratios)

def reference(hidden, head_proj, head_out, head_ratio, group_of, lengths, token_mask):
    mixture = head_mixture(head_ratio)
    proj_wide = head_proj.astype(jnp.float32)
    out_wide = head_out.astype(jnp.float32)

    def rollout_score(states):
        hidden_pre = jnp.einsum('ld,hdr->hlr', states.astype(jnp.float32), proj_wide)
        active = jnp.tanh(hidden_pre).astype(jnp.bfloat16)
        active = lax.optimization_barrier(active)
        scores = jnp.einsum('hlr,hr->hl', active.astype(jnp.float32), out_wide)
        return lax.optimization_barrier(jnp.sum(mixture[:, None] * scores, axis=0))
    combined = lax.map(rollout_score, hidden)
    positions = jnp.arange(LEN)
    last_mark = positions[None, :] == (lengths - 1)[:, None]
    reward = lax.optimization_barrier(jnp.sum(jnp.where(last_mark, combined, 0.0), axis=1))
    member = (group_of[:, None] == jnp.arange(GROUPS)[None, :]).astype(jnp.float32)
    group_mean = lax.optimization_barrier(jnp.sum(member * reward[:, None], axis=0)) / GROUP
    mean_rows = lax.optimization_barrier(jnp.sum(member * group_mean[None, :], axis=1))
    deviation = reward - mean_rows
    group_var = lax.optimization_barrier(jnp.sum(member * (deviation * deviation)[:, None], axis=0)) / GROUP
    group_best = lax.optimization_barrier(jnp.max(jnp.where(member > 0, reward[:, None], -jnp.inf), axis=0))
    var_rows = lax.optimization_barrier(jnp.sum(member * group_var[None, :], axis=1))
    best_rows = lax.optimization_barrier(jnp.sum(member * group_best[None, :], axis=1))
    shaped = (deviation / jnp.sqrt(var_rows + var_offset))[:, None] + token_weight * combined - gap_weight * (best_rows - reward)[:, None]
    valid_mask = (positions[None, :] < lengths[:, None]) & (token_mask == 1)
    return jnp.where(valid_mask, jnp.clip(shaped, -clip_limit, clip_limit), 0.0)
```

```python
import functools

import jax
import jax.numpy as jnp
from jax import lax
from jax.experimental import pallas as pl
from jax.experimental.pallas import tpu as pltpu
from jax.sharding import PartitionSpec as P

GROUP = 16
MESH = pl.DeviceIdType.MESH

token_weight = 0.5
gap_weight = 0.5
clip_limit = 2.0
var_offset = 0.04

ROW_PIECES = 4
DEPTH_PIECES = 2
PACK = 16


def kernel(
    chips,
    hidden, proj, readout, ratio, groups, lens, mask, out,
    rows_all, w_own, w_other, out_own, out_other, acc, comb, ends, msg, slots,
    ratio_s, groups_s, lens_s, groups_v, mask_v,
    row_sem, w_sem, small_sem, pair_send, pair_recv, all_send, all_recv,
):
    chip, core = lax.axis_index("dp"), lax.axis_index("head")
    width = hidden.shape[2]
    count, seq = mask.shape
    heads, _, rank = proj.shape
    devices = 2 * chips
    me = 2 * chip + core
    total_rows = count * seq
    piece = total_rows // ROW_PIECES
    blocks = piece // PACK
    depth = width // DEPTH_PIECES
    lanes = msg.shape[1]

    loads = [pltpu.make_async_copy(lens, lens_s, small_sem.at[0])]
    loads.append(pltpu.make_async_copy(ratio, ratio_s, small_sem.at[1]))
    loads.append(pltpu.make_async_copy(groups, groups_s, small_sem.at[2]))
    loads.append(pltpu.make_async_copy(readout, out_own, small_sem.at[3]))
    loads.append(pltpu.make_async_copy(groups, groups_v.at[0], small_sem.at[4]))
    loads.append(pltpu.make_async_copy(mask, mask_v, small_sem.at[5]))
    w_loads = [
        pltpu.make_async_copy(proj.at[k], w_own.at[:, pl.ds(k * rank, rank)], w_sem.at[k])
        for k in range(heads)
    ]
    h_loads = [
        pltpu.make_async_copy(
            hidden.at[pl.ds(m * blocks, blocks)],
            rows_all.at[pl.ds(m * blocks, blocks)],
            row_sem.at[m],
        )
        for m in range(ROW_PIECES)
    ]
    for copy in w_loads + h_loads + loads:
        copy.start()

    barrier = pltpu.get_barrier_semaphore()

    def greet(step, _):
        other = lax.rem(me + step, devices)
        pl.semaphore_signal(
            barrier, inc=1, device_id=(other // 2, lax.rem(other, 2)), device_id_type=MESH
        )
        return 0

    lax.fori_loop(1, devices, greet, 0)

    for copy in loads + w_loads:
        copy.wait()

    weights = [ratio_s[k].astype(jnp.float32) for k in range(2 * heads)]
    weight_sum = sum(weights[1:], weights[0])
    own_mix = [
        ratio_s[core * heads + k].astype(jnp.float32) / weight_sum for k in range(heads)
    ]
    other_mix = [
        ratio_s[(1 - core) * heads + k].astype(jnp.float32) / weight_sum for k in range(heads)
    ]

    def reader(values):
        wide = values[...].astype(jnp.float32)
        line = lax.broadcasted_iota(jnp.int32, (8, rank), 0)
        parts = [
            jnp.where(line == k, jnp.broadcast_to(wide[k : k + 1], (8, rank)), 0.0)
            for k in range(heads)
        ]
        return jnp.concatenate(parts, axis=1).astype(jnp.bfloat16)

    def scores(inner, lhs, mix):
        active = jnp.tanh(inner).astype(jnp.bfloat16)
        per_head = lax.dot_general(
            lhs, active, (((1,), (1,)), ((), ())), preferred_element_type=jnp.float32
        )
        line = mix[0] * per_head[0:1]
        for k in range(1, heads):
            line = line + mix[k] * per_head[k : k + 1]
        return line

    own_lhs = reader(out_own)

    def rows_of(m, cut):
        return rows_all[pl.ds(m * blocks, blocks), :, cut].reshape(piece, -1)

    def own_piece(m):
        at = pl.ds(m * piece, piece)
        inner = jnp.dot(rows_of(m, pl.ds(0, width)), w_own[...], preferred_element_type=jnp.float32)
        comb[:, at] = scores(inner, own_lhs, own_mix)

    for m in range(ROW_PIECES - 1):
        h_loads[m].wait()
        own_piece(m)
    h_loads[ROW_PIECES - 1].wait()

    sub = lax.broadcasted_iota(jnp.int32, (PACK, width), 0)
    picked = jnp.zeros((PACK, width), jnp.float32)
    for r in range(count):
        last = lens_s[r] - 1
        block = rows_all[r * (seq // PACK) + lax.div(last, PACK)].astype(jnp.float32)
        row = jnp.sum(jnp.where(sub == lax.rem(last, PACK), block, 0.0), axis=0, keepdims=True)
        picked = jnp.where(sub == r, jnp.broadcast_to(row, (PACK, width)), picked)
    ends[pl.ds(0, PACK), :] = picked.astype(jnp.bfloat16)

    pl.semaphore_wait(barrier, devices - 1)

    def to_pair(src, dst, k):
        return pltpu.make_async_remote_copy(
            src_ref=src, dst_ref=dst, send_sem=pair_send.at[k], recv_sem=pair_recv.at[k],
            device_id=(chip, 1 - core), device_id_type=MESH,
        )

    send_ends = to_pair(ends.at[pl.ds(0, PACK)], ends.at[pl.ds(PACK, PACK)], 0)
    send_out = to_pair(out_own, out_other, 1)
    send_w = [
        to_pair(w_own.at[pl.ds(d * depth, depth)], w_other.at[pl.ds(d * depth, depth)], 2 + d)
        for d in range(DEPTH_PIECES)
    ]
    send_ends.start()
    send_out.start()
    send_w[0].start()
    own_piece(ROW_PIECES - 1)
    send_ends.wait_recv()

    inner = jnp.dot(ends[...], w_own[...], preferred_element_type=jnp.float32)
    active = jnp.tanh(inner).astype(jnp.bfloat16).astype(jnp.float32)
    wide = out_own[...].astype(jnp.float32)
    scale = jnp.concatenate([own_mix[k] * wide[k : k + 1] for k in range(heads)], axis=1)
    part = jnp.sum(active * scale, axis=1, keepdims=True)
    line = lax.broadcasted_iota(jnp.int32, (2 * PACK, lanes), 0)
    lane = lax.broadcasted_iota(jnp.int32, (2 * PACK, lanes), 1)
    mine = (line < count) & (lane == me * count + line)
    theirs = (line >= PACK) & (line < PACK + count) & (
        lane == (4 * chip + 1 - me) * count + line - PACK
    )
    note = jnp.sum(jnp.where(mine | theirs, part, 0.0), axis=0, keepdims=True)
    msg[...] = note
    slots[me] = note

    def tell(step, _):
        other = lax.rem(me + step, devices)
        pltpu.make_async_remote_copy(
            src_ref=msg, dst_ref=slots.at[me], send_sem=all_send, recv_sem=all_recv,
            device_id=(other // 2, lax.rem(other, 2)), device_id_type=MESH,
        ).start()
        return 0

    lax.fori_loop(1, devices, tell, 0)
    for copy in send_w[1:]:
        copy.start()

    send_out.wait_recv()
    other_lhs = reader(out_other)
    for d in range(DEPTH_PIECES):
        send_w[d].wait_recv()
        cut = pl.ds(d * depth, depth)
        for m in range(ROW_PIECES):
            at = pl.ds(m * piece, piece)
            inner = jnp.dot(rows_of(m, cut), w_other[cut, :], preferred_element_type=jnp.float32)
            if d > 0:
                inner = acc[at, :] + inner
            if d < DEPTH_PIECES - 1:
                acc[at, :] = inner
            else:
                comb[:, at] = comb[:, at] + scores(inner, other_lhs, other_mix)

    rest = slots.at[pl.ds(0, devices - 1)]
    pltpu.make_async_copy(rest, rest, all_recv).wait()

    reward = jnp.sum(slots[...], axis=0)[:, : groups_v.shape[1]]
    labels = groups_v[...]
    spot = lax.broadcasted_iota(jnp.int32, reward.shape, 1)
    place = lax.broadcasted_iota(jnp.int32, (1, seq), 1)
    for r in range(count):
        index = me * count + r
        member = labels == groups_s[index]
        own = jnp.sum(jnp.where(spot == index, reward, 0.0), axis=1, keepdims=True)
        mean = jnp.sum(jnp.where(member, reward, 0.0), axis=1, keepdims=True) / GROUP
        gap = reward - mean
        var = jnp.sum(jnp.where(member, gap * gap, 0.0), axis=1, keepdims=True) / GROUP
        best = jnp.max(jnp.where(member, reward, -jnp.inf), axis=1, keepdims=True)
        base = (own - mean) / jnp.sqrt(var + var_offset) - gap_weight * (best - own)
        shaped = base + token_weight * comb[:, pl.ds(r * seq, seq)]
        valid = (place < lens_s[r]) & (mask_v[pl.ds(r, 1), :] == 1)
        out[pl.ds(r, 1), :] = jnp.where(valid, jnp.clip(shaped, -clip_limit, clip_limit), 0.0)

    send_ends.wait_send()
    send_out.wait_send()
    for copy in send_w:
        copy.wait_send()
    pltpu.make_async_copy(rest, rest, all_send).wait()


def solution(mesh):
    chips = mesh.shape["dp"]

    def on_device(hidden, head_proj, head_out, head_ratio, group_of, lengths, token_mask):
        count, seq, width = hidden.shape
        heads, _, rank = head_proj.shape
        everyone = group_of.shape[0]
        lanes = -(-everyone // 128) * 128
        hbm = pl.BlockSpec(memory_space=pltpu.HBM)
        bf16, f32, i32 = jnp.bfloat16, jnp.float32, jnp.int32
        return pl.pallas_call(
            functools.partial(kernel, chips),
            out_shape=jax.ShapeDtypeStruct((count, seq), f32),
            in_specs=[hbm] * 7,
            out_specs=pl.BlockSpec(memory_space=pltpu.VMEM),
            scratch_shapes=[
                pltpu.VMEM((count * seq // PACK, PACK, width), bf16),
                pltpu.VMEM((width, heads * rank), bf16),
                pltpu.VMEM((width, heads * rank), bf16),
                pltpu.VMEM((heads, rank), bf16),
                pltpu.VMEM((heads, rank), bf16),
                pltpu.VMEM((count * seq, heads * rank), f32),
                pltpu.VMEM((1, count * seq), f32),
                pltpu.VMEM((2 * PACK, width), bf16),
                pltpu.VMEM((1, lanes), f32),
                pltpu.VMEM((2 * chips, 1, lanes), f32),
                pltpu.SMEM(head_ratio.shape, i32),
                pltpu.SMEM(group_of.shape, i32),
                pltpu.SMEM(lengths.shape, i32),
                pltpu.VMEM((1, everyone), i32),
                pltpu.VMEM((count, seq), i32),
                pltpu.SemaphoreType.DMA((ROW_PIECES,)),
                pltpu.SemaphoreType.DMA((heads,)),
                pltpu.SemaphoreType.DMA((6,)),
                pltpu.SemaphoreType.DMA((2 + DEPTH_PIECES,)),
                pltpu.SemaphoreType.DMA((2 + DEPTH_PIECES,)),
                pltpu.SemaphoreType.DMA,
                pltpu.SemaphoreType.DMA,
            ],
            compiler_params=pltpu.CompilerParams(
                collective_id=0, has_side_effects=True, vmem_limit_bytes=60 * 1024 * 1024
            ),
            name="advantages",
        )(hidden.reshape(-1, PACK, width), head_proj, head_out, head_ratio, group_of, lengths, token_mask)

    return jax.shard_map(
        on_device,
        mesh=mesh,
        in_specs=(
            P(("dp", "head"), None, None),
            P("head", None, None),
            P("head", None),
            P(),
            P(),
            P(("dp", "head")),
            P(("dp", "head"), None),
        ),
        out_specs=P(("dp", "head"), None),
        check_vma=False,
    )
```

```python
import functools

import jax
import jax.numpy as jnp
from jax import lax
from jax.experimental import pallas as pl
from jax.experimental.pallas import tpu as pltpu
from jax.sharding import PartitionSpec as P

GROUP = 16
MESH = pl.DeviceIdType.MESH

token_weight = 0.5
gap_weight = 0.5
clip_limit = 2.0
var_offset = 0.04

DEPTH_PIECES = 2
PACK = 16


def kernel(
    chips,
    hidden, proj, readout, ratio, groups, lens, mask, out,
    rows_all, w_own, w_other, out_own, out_other, acc, comb, ends, msg, slots,
    ratio_s, groups_s, lens_s, groups_v, mask_v,
    row_sem, w_sem, small_sem, pair_send, pair_recv, all_send, all_recv,
):
    chip, core = lax.axis_index("dp"), lax.axis_index("head")
    width = hidden.shape[2]
    count, seq = mask.shape
    heads, _, rank = proj.shape
    devices = 2 * chips
    me = 2 * chip + core
    total_rows = count * seq
    depth = width // DEPTH_PIECES
    lanes = msg.shape[1]

    loads = [pltpu.make_async_copy(lens, lens_s, small_sem.at[0])]
    loads.append(pltpu.make_async_copy(ratio, ratio_s, small_sem.at[1]))
    loads.append(pltpu.make_async_copy(groups, groups_s, small_sem.at[2]))
    loads.append(pltpu.make_async_copy(readout, out_own, small_sem.at[3]))
    loads.append(pltpu.make_async_copy(groups, groups_v.at[0], small_sem.at[4]))
    loads.append(pltpu.make_async_copy(mask, mask_v, small_sem.at[5]))
    w_loads = [
        pltpu.make_async_copy(proj.at[k], w_own.at[:, pl.ds(k * rank, rank)], w_sem.at[k])
        for k in range(heads)
    ]
    cuts = [pl.ds(d * depth, depth) for d in range(DEPTH_PIECES)]
    h_loads = [
        pltpu.make_async_copy(hidden.at[:, :, cuts[d]], rows_all.at[:, :, cuts[d]], row_sem.at[d])
        for d in range(DEPTH_PIECES)
    ]
    for copy in w_loads + h_loads + loads:
        copy.start()

    barrier = pltpu.get_barrier_semaphore()

    def greet(step, _):
        other = lax.rem(me + step, devices)
        pl.semaphore_signal(
            barrier, inc=1, device_id=(other // 2, lax.rem(other, 2)), device_id_type=MESH
        )
        return 0

    lax.fori_loop(1, devices, greet, 0)

    for copy in loads + w_loads:
        copy.wait()

    weights = [ratio_s[k].astype(jnp.float32) for k in range(2 * heads)]
    weight_sum = sum(weights[1:], weights[0])
    own_mix = [
        ratio_s[core * heads + k].astype(jnp.float32) / weight_sum for k in range(heads)
    ]
    other_mix = [
        ratio_s[(1 - core) * heads + k].astype(jnp.float32) / weight_sum for k in range(heads)
    ]

    def reader(values):
        wide = values[...].astype(jnp.float32)
        line = lax.broadcasted_iota(jnp.int32, (8, rank), 0)
        parts = [
            jnp.where(line == k, jnp.broadcast_to(wide[k : k + 1], (8, rank)), 0.0)
            for k in range(heads)
        ]
        return jnp.concatenate(parts, axis=1).astype(jnp.bfloat16)

    def scores(inner, lhs, mix):
        active = jnp.tanh(inner).astype(jnp.bfloat16)
        per_head = lax.dot_general(
            lhs, active, (((1,), (1,)), ((), ())), preferred_element_type=jnp.float32
        )
        line = mix[0] * per_head[0:1]
        for k in range(1, heads):
            line = line + mix[k] * per_head[k : k + 1]
        return line

    own_lhs = reader(out_own)

    def partial(values, d):
        rows = rows_all[:, :, cuts[d]].reshape(total_rows, depth)
        return jnp.dot(rows, values[cuts[d], :], preferred_element_type=jnp.float32)

    def add_partial(values, d):
        inner = partial(values, d)
        if d > 0:
            inner = acc[...] + inner
        if d < DEPTH_PIECES - 1:
            acc[...] = inner
        return inner

    for d in range(DEPTH_PIECES - 1):
        h_loads[d].wait()
        add_partial(w_own, d)
    h_loads[DEPTH_PIECES - 1].wait()

    sub = lax.broadcasted_iota(jnp.int32, (PACK, width), 0)
    picked = jnp.zeros((PACK, width), jnp.float32)
    for r in range(count):
        last = lens_s[r] - 1
        block = rows_all[r * (seq // PACK) + lax.div(last, PACK)].astype(jnp.float32)
        row = jnp.sum(jnp.where(sub == lax.rem(last, PACK), block, 0.0), axis=0, keepdims=True)
        picked = jnp.where(sub == r, jnp.broadcast_to(row, (PACK, width)), picked)
    ends[pl.ds(0, PACK), :] = picked.astype(jnp.bfloat16)

    pl.semaphore_wait(barrier, devices - 1)

    def to_pair(src, dst, k):
        return pltpu.make_async_remote_copy(
            src_ref=src, dst_ref=dst, send_sem=pair_send.at[k], recv_sem=pair_recv.at[k],
            device_id=(chip, 1 - core), device_id_type=MESH,
        )

    send_ends = to_pair(ends.at[pl.ds(0, PACK)], ends.at[pl.ds(PACK, PACK)], 0)
    send_out = to_pair(out_own, out_other, 1)
    send_w = [
        to_pair(w_own.at[cuts[d]], w_other.at[cuts[d]], 2 + d)
        for d in range(DEPTH_PIECES)
    ]
    send_ends.start()
    send_out.start()
    send_w[0].start()
    comb[...] = scores(add_partial(w_own, DEPTH_PIECES - 1), own_lhs, own_mix)
    send_ends.wait_recv()

    inner = jnp.dot(ends[...], w_own[...], preferred_element_type=jnp.float32)
    active = jnp.tanh(inner).astype(jnp.bfloat16).astype(jnp.float32)
    wide = out_own[...].astype(jnp.float32)
    scale = jnp.concatenate([own_mix[k] * wide[k : k + 1] for k in range(heads)], axis=1)
    part = jnp.sum(active * scale, axis=1, keepdims=True)
    line = lax.broadcasted_iota(jnp.int32, (2 * PACK, lanes), 0)
    lane = lax.broadcasted_iota(jnp.int32, (2 * PACK, lanes), 1)
    mine = (line < count) & (lane == me * count + line)
    theirs = (line >= PACK) & (line < PACK + count) & (
        lane == (4 * chip + 1 - me) * count + line - PACK
    )
    note = jnp.sum(jnp.where(mine | theirs, part, 0.0), axis=0, keepdims=True)
    msg[...] = note
    slots[me] = note

    def tell(step, _):
        other = lax.rem(me + step, devices)
        pltpu.make_async_remote_copy(
            src_ref=msg, dst_ref=slots.at[me], send_sem=all_send, recv_sem=all_recv,
            device_id=(other // 2, lax.rem(other, 2)), device_id_type=MESH,
        ).start()
        return 0

    lax.fori_loop(1, devices, tell, 0)
    for copy in send_w[1:]:
        copy.start()

    send_out.wait_recv()
    other_lhs = reader(out_other)
    for d in range(DEPTH_PIECES):
        send_w[d].wait_recv()
        inner = add_partial(w_other, d)
    comb[...] = comb[...] + scores(inner, other_lhs, other_mix)

    rest = slots.at[pl.ds(0, devices - 1)]
    pltpu.make_async_copy(rest, rest, all_recv).wait()

    reward = jnp.sum(slots[...], axis=0)[:, : groups_v.shape[1]]
    labels = groups_v[...]
    spot = lax.broadcasted_iota(jnp.int32, reward.shape, 1)
    place = lax.broadcasted_iota(jnp.int32, (1, seq), 1)
    for r in range(count):
        index = me * count + r
        member = labels == groups_s[index]
        own = jnp.sum(jnp.where(spot == index, reward, 0.0), axis=1, keepdims=True)
        mean = jnp.sum(jnp.where(member, reward, 0.0), axis=1, keepdims=True) / GROUP
        gap = reward - mean
        var = jnp.sum(jnp.where(member, gap * gap, 0.0), axis=1, keepdims=True) / GROUP
        best = jnp.max(jnp.where(member, reward, -jnp.inf), axis=1, keepdims=True)
        base = (own - mean) / jnp.sqrt(var + var_offset) - gap_weight * (best - own)
        shaped = base + token_weight * comb[:, pl.ds(r * seq, seq)]
        valid = (place < lens_s[r]) & (mask_v[pl.ds(r, 1), :] == 1)
        out[pl.ds(r, 1), :] = jnp.where(valid, jnp.clip(shaped, -clip_limit, clip_limit), 0.0)

    send_ends.wait_send()
    send_out.wait_send()
    for copy in send_w:
        copy.wait_send()
    pltpu.make_async_copy(rest, rest, all_send).wait()


def solution(mesh):
    chips = mesh.shape["dp"]

    def on_device(hidden, head_proj, head_out, head_ratio, group_of, lengths, token_mask):
        count, seq, width = hidden.shape
        heads, _, rank = head_proj.shape
        everyone = group_of.shape[0]
        lanes = -(-everyone // 128) * 128
        hbm = pl.BlockSpec(memory_space=pltpu.HBM)
        bf16, f32, i32 = jnp.bfloat16, jnp.float32, jnp.int32
        return pl.pallas_call(
            functools.partial(kernel, chips),
            out_shape=jax.ShapeDtypeStruct((count, seq), f32),
            in_specs=[hbm] * 7,
            out_specs=pl.BlockSpec(memory_space=pltpu.VMEM),
            scratch_shapes=[
                pltpu.VMEM((count * seq // PACK, PACK, width), bf16),
                pltpu.VMEM((width, heads * rank), bf16),
                pltpu.VMEM((width, heads * rank), bf16),
                pltpu.VMEM((heads, rank), bf16),
                pltpu.VMEM((heads, rank), bf16),
                pltpu.VMEM((count * seq, heads * rank), f32),
                pltpu.VMEM((1, count * seq), f32),
                pltpu.VMEM((2 * PACK, width), bf16),
                pltpu.VMEM((1, lanes), f32),
                pltpu.VMEM((2 * chips, 1, lanes), f32),
                pltpu.SMEM(head_ratio.shape, i32),
                pltpu.SMEM(group_of.shape, i32),
                pltpu.SMEM(lengths.shape, i32),
                pltpu.VMEM((1, everyone), i32),
                pltpu.VMEM((count, seq), i32),
                pltpu.SemaphoreType.DMA((DEPTH_PIECES,)),
                pltpu.SemaphoreType.DMA((heads,)),
                pltpu.SemaphoreType.DMA((6,)),
                pltpu.SemaphoreType.DMA((2 + DEPTH_PIECES,)),
                pltpu.SemaphoreType.DMA((2 + DEPTH_PIECES,)),
                pltpu.SemaphoreType.DMA,
                pltpu.SemaphoreType.DMA,
            ],
            compiler_params=pltpu.CompilerParams(
                collective_id=0, has_side_effects=True, vmem_limit_bytes=60 * 1024 * 1024
            ),
            name="advantages",
        )(hidden.reshape(-1, PACK, width), head_proj, head_out, head_ratio, group_of, lengths, token_mask)

    return jax.shard_map(
        on_device,
        mesh=mesh,
        in_specs=(
            P(("dp", "head"), None, None),
            P("head", None, None),
            P("head", None),
            P(),
            P(),
            P(("dp", "head")),
            P(("dp", "head"), None),
        ),
        out_specs=P(("dp", "head"), None),
        check_vma=False,
    )
```

```python
import functools

import jax
import jax.numpy as jnp
from jax import lax
from jax.experimental import pallas as pl
from jax.experimental.pallas import tpu as pltpu
from jax.sharding import PartitionSpec as P

GROUP = 16
MESH = pl.DeviceIdType.MESH

token_weight = 0.5
gap_weight = 0.5
clip_limit = 2.0
var_offset = 0.04

DEPTH_PIECES = 2
PACK = 16


def kernel(
    chips,
    hidden, proj, readout, ratio, groups, lens, mask, out,
    rows_all, w_own, w_other, out_own, out_other, acc, comb, ends, msg, slots,
    ratio_s, groups_s, lens_s, groups_v, mask_v,
    row_sem, w_sem, small_sem, pair_send, pair_recv, all_send, all_recv,
):
    chip, core = lax.axis_index("dp"), lax.axis_index("head")
    width = hidden.shape[2]
    count, seq = mask.shape
    heads, _, rank = proj.shape
    devices = 2 * chips
    me = 2 * chip + core
    total_rows = count * seq
    depth = width // DEPTH_PIECES
    lanes = msg.shape[1]

    loads = [pltpu.make_async_copy(lens, lens_s, small_sem.at[0])]
    loads.append(pltpu.make_async_copy(ratio, ratio_s, small_sem.at[1]))
    loads.append(pltpu.make_async_copy(groups, groups_s, small_sem.at[2]))
    loads.append(pltpu.make_async_copy(readout, out_own, small_sem.at[3]))
    loads.append(pltpu.make_async_copy(groups, groups_v.at[0], small_sem.at[4]))
    loads.append(pltpu.make_async_copy(mask, mask_v, small_sem.at[5]))
    w_loads = [
        pltpu.make_async_copy(proj.at[k], w_own.at[:, pl.ds(k * rank, rank)], w_sem.at[k])
        for k in range(heads)
    ]
    cuts = [pl.ds(d * depth, depth) for d in range(DEPTH_PIECES)]
    h_loads = [
        pltpu.make_async_copy(hidden.at[:, :, cuts[d]], rows_all.at[:, :, cuts[d]], row_sem.at[d])
        for d in range(DEPTH_PIECES)
    ]
    for copy in loads[:1] + h_loads + w_loads + loads[1:]:
        copy.start()

    barrier = pltpu.get_barrier_semaphore()

    def each_other(act):
        def both(step, _):
            there = lax.rem(chip + step, chips)
            act((there, core))
            act((there, 1 - core))
            return 0

        if chips <= 16:
            for step in range(1, chips):
                both(step, 0)
        else:
            lax.fori_loop(1, chips, both, 0)
        act((chip, 1 - core))

    each_other(
        lambda place: pl.semaphore_signal(barrier, inc=1, device_id=place, device_id_type=MESH)
    )

    for copy in loads[:1] + h_loads:
        copy.wait()

    sub = lax.broadcasted_iota(jnp.int32, (PACK, width), 0)
    picked = jnp.zeros((PACK, width), jnp.float32)
    for r in range(count):
        last = lens_s[r] - 1
        block = rows_all[r * (seq // PACK) + lax.div(last, PACK)].astype(jnp.float32)
        row = jnp.sum(jnp.where(sub == lax.rem(last, PACK), block, 0.0), axis=0, keepdims=True)
        picked = jnp.where(sub == r, jnp.broadcast_to(row, (PACK, width)), picked)
    ends[pl.ds(0, PACK), :] = picked.astype(jnp.bfloat16)

    pl.semaphore_wait(barrier, devices - 1)

    def to_pair(src, dst, k):
        return pltpu.make_async_remote_copy(
            src_ref=src, dst_ref=dst, send_sem=pair_send.at[k], recv_sem=pair_recv.at[k],
            device_id=(chip, 1 - core), device_id_type=MESH,
        )

    send_ends = to_pair(ends.at[pl.ds(0, PACK)], ends.at[pl.ds(PACK, PACK)], 0)
    send_out = to_pair(out_own, out_other, 1)
    send_w = [
        to_pair(w_own.at[cuts[d]], w_other.at[cuts[d]], 2 + d)
        for d in range(DEPTH_PIECES)
    ]
    send_ends.start()
    for copy in w_loads + loads[1:]:
        copy.wait()
    send_out.start()
    send_w[0].start()

    weights = [ratio_s[k].astype(jnp.float32) for k in range(2 * heads)]
    weight_sum = sum(weights[1:], weights[0])
    own_mix = [
        ratio_s[core * heads + k].astype(jnp.float32) / weight_sum for k in range(heads)
    ]
    other_mix = [
        ratio_s[(1 - core) * heads + k].astype(jnp.float32) / weight_sum for k in range(heads)
    ]

    def reader(values):
        wide = values[...].astype(jnp.float32)
        line = lax.broadcasted_iota(jnp.int32, (8, rank), 0)
        parts = [
            jnp.where(line == k, jnp.broadcast_to(wide[k : k + 1], (8, rank)), 0.0)
            for k in range(heads)
        ]
        return jnp.concatenate(parts, axis=1).astype(jnp.bfloat16)

    def scores(inner, lhs, mix):
        active = jnp.tanh(inner).astype(jnp.bfloat16)
        per_head = lax.dot_general(
            lhs, active, (((1,), (1,)), ((), ())), preferred_element_type=jnp.float32
        )
        line = mix[0] * per_head[0:1]
        for k in range(1, heads):
            line = line + mix[k] * per_head[k : k + 1]
        return line

    own_lhs = reader(out_own)

    def partial(values, d):
        rows = rows_all[:, :, cuts[d]].reshape(total_rows, depth)
        return jnp.dot(rows, values[cuts[d], :], preferred_element_type=jnp.float32)

    def add_partial(values, d):
        inner = partial(values, d)
        if d > 0:
            inner = acc[...] + inner
        if d < DEPTH_PIECES - 1:
            acc[...] = inner
        return inner

    add_partial(w_own, 0)
    send_ends.wait_recv()

    inner = jnp.dot(ends[...], w_own[...], preferred_element_type=jnp.float32)
    active = jnp.tanh(inner).astype(jnp.bfloat16).astype(jnp.float32)
    wide = out_own[...].astype(jnp.float32)
    scale = jnp.concatenate([own_mix[k] * wide[k : k + 1] for k in range(heads)], axis=1)
    part = jnp.sum(active * scale, axis=1, keepdims=True)
    line = lax.broadcasted_iota(jnp.int32, (2 * PACK, lanes), 0)
    lane = lax.broadcasted_iota(jnp.int32, (2 * PACK, lanes), 1)
    mine = (line < count) & (lane == me * count + line)
    theirs = (line >= PACK) & (line < PACK + count) & (
        lane == (4 * chip + 1 - me) * count + line - PACK
    )
    note = jnp.sum(jnp.where(mine | theirs, part, 0.0), axis=0, keepdims=True)
    msg[...] = note
    slots[me] = note

    each_other(
        lambda place: pltpu.make_async_remote_copy(
            src_ref=msg, dst_ref=slots.at[me], send_sem=all_send, recv_sem=all_recv,
            device_id=place, device_id_type=MESH,
        ).start()
    )
    for copy in send_w[1:]:
        copy.start()

    for d in range(1, DEPTH_PIECES):
        inner = add_partial(w_own, d)
    comb[...] = scores(inner, own_lhs, own_mix)

    send_out.wait_recv()
    other_lhs = reader(out_other)
    for d in range(DEPTH_PIECES):
        send_w[d].wait_recv()
        inner = add_partial(w_other, d)
    comb[...] = comb[...] + scores(inner, other_lhs, other_mix)

    rest = slots.at[pl.ds(0, devices - 1)]
    pltpu.make_async_copy(rest, rest, all_recv).wait()

    reward = jnp.sum(slots[...], axis=0)[:, : groups_v.shape[1]]
    labels = groups_v[...]
    shape = (count, reward.shape[1])
    rollout = lax.broadcasted_iota(jnp.int32, shape, 0)
    lane_of = lax.broadcasted_iota(jnp.int32, shape, 1)
    wide = jnp.broadcast_to(reward, shape)
    group = jnp.zeros(shape, jnp.int32)
    length = jnp.zeros((count, seq), jnp.int32)
    line = lax.broadcasted_iota(jnp.int32, (count, seq), 0)
    for r in range(count):
        group = jnp.where(rollout == r, groups_s[me * count + r], group)
        length = jnp.where(line == r, lens_s[r], length)
    member = jnp.broadcast_to(labels, shape) == group
    own = jnp.sum(jnp.where(lane_of == me * count + rollout, wide, 0.0), axis=1, keepdims=True)
    mean = jnp.sum(jnp.where(member, wide, 0.0), axis=1, keepdims=True) / GROUP
    gap = wide - mean
    var = jnp.sum(jnp.where(member, gap * gap, 0.0), axis=1, keepdims=True) / GROUP
    best = jnp.max(jnp.where(member, wide, -jnp.inf), axis=1, keepdims=True)
    base = (own - mean) / jnp.sqrt(var + var_offset) - gap_weight * (best - own)
    shaped = base + token_weight * jnp.concatenate(
        [comb[:, pl.ds(r * seq, seq)] for r in range(count)], axis=0
    )
    place = lax.broadcasted_iota(jnp.int32, (count, seq), 1)
    valid = (place < length) & (mask_v[...] == 1)
    out[...] = jnp.where(valid, jnp.clip(shaped, -clip_limit, clip_limit), 0.0)

    send_ends.wait_send()
    send_out.wait_send()
    for copy in send_w:
        copy.wait_send()
    pltpu.make_async_copy(rest, rest, all_send).wait()


def solution(mesh):
    chips = mesh.shape["dp"]

    def on_device(hidden, head_proj, head_out, head_ratio, group_of, lengths, token_mask):
        count, seq, width = hidden.shape
        heads, _, rank = head_proj.shape
        everyone = group_of.shape[0]
        lanes = -(-everyone // 128) * 128
        hbm = pl.BlockSpec(memory_space=pltpu.HBM)
        bf16, f32, i32 = jnp.bfloat16, jnp.float32, jnp.int32
        return pl.pallas_call(
            functools.partial(kernel, chips),
            out_shape=jax.ShapeDtypeStruct((count, seq), f32),
            in_specs=[hbm] * 7,
            out_specs=pl.BlockSpec(memory_space=pltpu.VMEM),
            scratch_shapes=[
                pltpu.VMEM((count * seq // PACK, PACK, width), bf16),
                pltpu.VMEM((width, heads * rank), bf16),
                pltpu.VMEM((width, heads * rank), bf16),
                pltpu.VMEM((heads, rank), bf16),
                pltpu.VMEM((heads, rank), bf16),
                pltpu.VMEM((count * seq, heads * rank), f32),
                pltpu.VMEM((1, count * seq), f32),
                pltpu.VMEM((2 * PACK, width), bf16),
                pltpu.VMEM((1, lanes), f32),
                pltpu.VMEM((2 * chips, 1, lanes), f32),
                pltpu.SMEM(head_ratio.shape, i32),
                pltpu.SMEM(group_of.shape, i32),
                pltpu.SMEM(lengths.shape, i32),
                pltpu.VMEM((1, everyone), i32),
                pltpu.VMEM((count, seq), i32),
                pltpu.SemaphoreType.DMA((DEPTH_PIECES,)),
                pltpu.SemaphoreType.DMA((heads,)),
                pltpu.SemaphoreType.DMA((6,)),
                pltpu.SemaphoreType.DMA((2 + DEPTH_PIECES,)),
                pltpu.SemaphoreType.DMA((2 + DEPTH_PIECES,)),
                pltpu.SemaphoreType.DMA,
                pltpu.SemaphoreType.DMA,
            ],
            compiler_params=pltpu.CompilerParams(
                collective_id=0, has_side_effects=True, vmem_limit_bytes=60 * 1024 * 1024
            ),
            name="advantages",
        )(hidden.reshape(-1, PACK, width), head_proj, head_out, head_ratio, group_of, lengths, token_mask)

    return jax.shard_map(
        on_device,
        mesh=mesh,
        in_specs=(
            P(("dp", "head"), None, None),
            P("head", None, None),
            P("head", None),
            P(),
            P(),
            P(("dp", "head")),
            P(("dp", "head"), None),
        ),
        out_specs=P(("dp", "head"), None),
        check_vma=False,
    )
```
